32 devices in a mesh: depth: 8 (over z, y), height: 2 (over core), view: 2 (over x).
Axes of the slice: x: 2, y: 2, z: 4, core: 2. Of those that a mesh axis runs over, the one named last changes fastest.
Arguments:
- camera_feats: bfloat16 [256, 16, 128], P(('depth', 'height', 'view')), may hold values from -6 to 6
- footprint_slot_weights: bfloat16 [8, 128, 128], replicated, may hold values from -0.1875 to 0.1875
- tile_bricks: int32 [256, 8], P(('depth', 'height', 'view')), may hold values from 0 to 1
- tile_rows: int32 [256, 8], P(('depth', 'height', 'view')), may hold values from 0 to 7
- conv_first: bfloat16 [16, 16, 3, 3, 3], replicated, may hold values from -0.3125 to 0.3125
- conv_second: bfloat16 [16, 16, 3, 3, 3], replicated, may hold values from -0.3125 to 0.3125
- conv_third: bfloat16 [16, 16, 3, 3, 3], replicated, may hold values from -0.3125 to 0.3125
- bias_first: float32 [16], replicated, may hold values from -3 to 3
- bias_second: float32 [16], replicated, may hold values from -3 to 3
- out_grad: bfloat16 [16, 16, 16, 128], P(('depth', 'view'), 'height'), may hold values from -6 to 6
Outputs:
- field: bfloat16 [16, 16, 16, 128], P(('depth', 'view'), 'height')
- camera_tile_feature_gradient: float32 [256, 16, 128], P(('depth', 'height', 'view'))
- weight_grads: float32 [3, 16, 16, 3, 3, 3], replicated
- bias_gradient_pair: float32 [2, 16], replicated
The draws below stay inside these ranges and needn't reach their ends.
All inputs are finite; a program needn't handle non-finite values.
Results may differ from the reference program's by a relative error of at most 0.017.
Values may be sent and summed in bfloat16 or wider, within the bound.
A program may use at most 64 MiB of HBM per device.

```python
import math
import jax
import jax.numpy as jnp
from jax import lax

C = 16
P_SIZE = 128
XB = 128
K = 8
ZP = 1
CX = 128
CY = 8
TILES = 8
NZ = 16
NY = 16
NX = 128
CAMTILES = 256
N_DEPTH = 8
N_HEIGHT = 2
N_VIEW = 2


def draw_out_grad(key, part):
    random_key_first = jax.random.fold_in(jax.random.fold_in(key, 11), 0)
    depth_pos = jnp.arange(NZ, dtype=jnp.float32) / max(NZ - 1, 1)
    scaling = (0.5 + depth_pos)[:, None, None, None]
    noise_part = jnp.clip(jax.random.normal(random_key_first, (NZ, NY, C, NX), jnp.float32), -4.0, 4.0)
    drawn = noise_part * scaling
    return drawn.astype(jnp.bfloat16)


def with_ends(values, stream_key, least, largest):
    shape = values.shape
    place = [jax.random.randint(jax.random.fold_in(stream_key, axis), (), 0, shape[axis]) for axis in range(len(shape))]
    values = values.at[tuple(place)].set(least)
    longest = shape.index(max(shape))
    place[longest] = (place[longest] + 1) % shape[longest]
    return values.at[tuple(place)].set(largest)


def steps_of(key, extent, pieces, least, largest):
    gain, own = 1.0, jax.random.fold_in(key, 6)
    for position, shards_of in pieces:
        draws = jnp.exp(jax.random.uniform(jax.random.fold_in(own, position), (shards_of,), jnp.float32, least / len(pieces), largest / len(pieces)))
        gain = gain * jnp.repeat(draws, extent[position] // shards_of).reshape([-1 if axis == position else 1 for axis in range(len(extent))])
    return gain


def centred(key, extent, deviation, most, shards=(), held_as=jnp.bfloat16):
    entries = deviation * jax.random.normal(key, extent, jnp.float32)
    if shards:
        entries = entries * steps_of(key, extent, shards, -0.22, 0.18)
    return jnp.clip(entries, -most, most).astype(held_as)


def setup_inputs(seed: int = 0) -> dict:
    streams_of = jax.random.split(jax.random.key(seed), 11)
    return {
        "camera_feats": centred(streams_of[0], (CAMTILES, C, P_SIZE), 1.0, 6.0, ((0, 32),)),
        "footprint_slot_weights": centred(streams_of[1], (K, XB, P_SIZE), (TILES * K * P_SIZE // (ZP * CY * CX // XB)) ** -0.5, 0.1875),
        "tile_bricks": with_ends(jax.random.randint(streams_of[2], (CAMTILES, K), 0, N_VIEW), jax.random.fold_in(streams_of[2], 1), 0, N_VIEW - 1).astype(jnp.int32),
        "tile_rows": with_ends(jax.random.randint(streams_of[3], (CAMTILES, K), 0, ZP * CY * CX // XB), jax.random.fold_in(streams_of[3], 1), 0, (ZP * CY * CX // XB) - 1).astype(jnp.int32),
        "conv_first": centred(streams_of[4], (C, C, 3, 3, 3), (27 * C) ** -0.5, 0.3125),
        "conv_second": centred(streams_of[5], (C, C, 3, 3, 3), (27 * C) ** -0.5, 0.3125),
        "conv_third": centred(streams_of[6], (C, C, 3, 3, 3), (27 * C) ** -0.5, 0.3125),
        "bias_first": centred(streams_of[7], (C,), 0.5, 3.0, (), jnp.float32),
        "bias_second": centred(streams_of[8], (C,), 0.5, 3.0, (), jnp.float32),
        "out_grad": draw_out_grad(jax.random.fold_in(streams_of[10], 71), 0),
    }


conv_layout = ('NDHCW', 'OIDHW', 'NDHCW')
grad_layout = ('CDHNW', 'IDHOW', 'CNDHW')

def conv_same(volume, weight):
    result = lax.conv_general_dilated(volume[None], weight, (1, 1, 1), ((1, 1), (1, 1), (1, 1)), dimension_numbers=conv_layout, preferred_element_type=jnp.float32)
    return result[0]

def flip_swap(weight):
    return jnp.transpose(jnp.flip(weight, (2, 3, 4)), (1, 0, 2, 3, 4))

def weight_grad(grad_out, volume):
    padded = jnp.pad(volume, ((1, 1), (1, 1), (0, 0), (1, 1)))
    return lax.conv_general_dilated(padded[None], grad_out[None], (1, 1, 1), ((0, 0), (0, 0), (0, 0)), dimension_numbers=grad_layout, preferred_element_type=jnp.float32)

def silu_grad(values):
    sigma = jax.nn.sigmoid(values)
    return sigma * (1.0 + values * (1.0 - sigma))

def lift_region(region_feature_slab, bricks_region, rows_region, footprint_slot_weights):
    block_count = CX // XB
    plane_rows = bricks_region * (ZP * CY) + rows_region // block_count
    blocks = rows_region % block_count
    view_ids = jnp.arange(N_VIEW, dtype=jnp.int32)[:, None, None]
    partial_value = jnp.zeros((N_VIEW, N_VIEW * ZP * CY, C, block_count, XB), jnp.float32)
    contrib = jnp.einsum('vtcp,kxp->vtkcx', region_feature_slab.astype(jnp.float32), footprint_slot_weights.astype(jnp.float32))
    partial_value = partial_value.at[view_ids, plane_rows, :, blocks, :].add(contrib)
    rounded = lax.optimization_barrier(partial_value.astype(jnp.bfloat16)).astype(jnp.float32)
    region = lax.optimization_barrier(jnp.sum(rounded, axis=0)).astype(jnp.bfloat16)
    return region.reshape(N_VIEW * ZP, CY, C, CX)

def reference(camera_feats, footprint_slot_weights, tile_bricks, tile_rows, conv_first, conv_second, conv_third, bias_first, bias_second, out_grad):
    regions_count = N_DEPTH * N_HEIGHT
    feature_partition = camera_feats.reshape(regions_count, N_VIEW, TILES, C, P_SIZE)
    bricks_split = tile_bricks.reshape(regions_count, N_VIEW, TILES, K)
    rows_split = tile_rows.reshape(regions_count, N_VIEW, TILES, K)
    regions = lax.map(lambda items: lift_region(items[0], items[1], items[2], footprint_slot_weights), (feature_partition, bricks_split, rows_split))
    lifted = jnp.transpose(regions.reshape(N_DEPTH, N_HEIGHT, N_VIEW * ZP, CY, C, CX), (0, 2, 1, 3, 4, 5)).reshape(NZ, NY, C, CX)
    pre_first = conv_same(lifted, conv_first) + bias_first[None, None, :, None]
    act_first = jax.nn.silu(pre_first).astype(jnp.bfloat16)
    pre_second = conv_same(act_first, conv_second) + bias_second[None, None, :, None]
    act_second = (jax.nn.silu(pre_second) + act_first.astype(jnp.float32)).astype(jnp.bfloat16)
    field = conv_same(act_second, conv_third).astype(jnp.bfloat16)
    up_second = conv_same(out_grad, flip_swap(conv_third))
    slope_second = up_second * silu_grad(pre_second)
    back_second = slope_second.astype(jnp.bfloat16)
    up_first = up_second + conv_same(back_second, flip_swap(conv_second))
    slope_first = up_first * silu_grad(pre_first)
    back_first = slope_first.astype(jnp.bfloat16)
    lift_grad = conv_same(back_first, flip_swap(conv_first)).astype(jnp.bfloat16)
    block_count = CX // XB
    device_ids = jnp.arange(CAMTILES, dtype=jnp.int32) // TILES
    region_ids = device_ids // N_VIEW
    depth_ids = region_ids // N_HEIGHT
    height_index_list = region_ids % N_HEIGHT
    planes = (depth_ids[:, None] * N_VIEW + tile_bricks) * ZP + tile_rows // (CY * block_count)
    ycells = height_index_list[:, None] * CY + tile_rows // block_count % CY
    blocks = tile_rows % block_count
    grid = lift_grad.reshape(NZ, NY, C, block_count, XB)
    chosen_table_entries = grid[planes, ycells, :, blocks, :]
    camera_tile_feature_gradient = jnp.einsum('urvo,ron->uvn', chosen_table_entries.astype(jnp.float32), footprint_slot_weights.astype(jnp.float32))
    scale = 1.0 / math.sqrt(NZ * NY * NX)
    weight_grads = jnp.stack([weight_grad(back_first, lifted), weight_grad(back_second, act_first), weight_grad(out_grad, act_second)]) * scale
    bias_gradient_pair = jnp.stack([lax.optimization_barrier(jnp.sum(slope_first, axis=(0, 1, 3))), lax.optimization_barrier(jnp.sum(slope_second, axis=(0, 1, 3)))]) * scale
    return (field, camera_tile_feature_gradient, weight_grads, bias_gradient_pair)
```

```python
import math

import jax
import jax.numpy as jnp
from jax import lax
from jax.experimental import pallas as pl
from jax.experimental.pallas import tpu as pltpu
from jax.sharding import PartitionSpec as P

MESH = pl.DeviceIdType.MESH
F32 = jnp.float32
BF16 = jnp.bfloat16
DIRS = [(dz, dy) for dz in (-1, 0, 1) for dy in (0, -1, 1) if (dz, dy) != (0, 0)]
LIFT, ACT1, ACT2, OUTG, BACK2, BACK1 = range(6)
BIAS_ROWS = 16


def round_up(value, step):
    return -(-value // step) * step


def silu_grad(values):
    sigma = jax.nn.sigmoid(values)
    return sigma * (1.0 + values * (1.0 - sigma))


def make_kernel(depths, heights, views, tiles, slots, rows_y, channels, width):
    group = heights * views
    wrows = 9 * channels
    srows = 3 * channels
    cells = rows_y * channels
    total_rows = wrows + BIAS_ROWS
    piece = round_up(-(-total_rows // depths), 8)

    def kernel(
        bricks_ref, rows_ref, feats_ref, foot_ref, w_ref, bias_ref, outg_ref,
        field_ref, camera_ref, early_out, late_out,
        vol, part, rsbuf, grid, own_sum, ar_rs, ar_mid,
        halo_send, halo_recv, view_send, view_recv, ar_send, ar_recv,
    ):
        d = lax.axis_index("depth")
        h = lax.axis_index("height")
        v = lax.axis_index("view")
        z = d * views + v
        planes = depths * views

        def exists(dz, dy):
            tests = []
            if dz == -1:
                tests.append(z > 0)
            if dz == 1:
                tests.append(z < planes - 1)
            if dy == -1:
                tests.append(h > 0)
            if dy == 1:
                tests.append(h < heights - 1)
            result = tests[0]
            for test in tests[1:]:
                result = jnp.logical_and(result, test)
            return result

        def neighbour(dz, dy):
            to = z + dz
            return {"depth": lax.div(to, views), "view": lax.rem(to, views), "height": h + dy}

        def halo_slot(index, dz, dy):
            if dy == 0:
                return vol.at[index, 1 - dz, pl.ds(1, rows_y)]
            return vol.at[index, 1 - dz, pl.ds(0 if dy == 1 else rows_y + 1, 1)]

        def halo_source(index, dy):
            base = vol.at[index, 1]
            if dy == 0:
                return base.at[pl.ds(1, rows_y)]
            return base.at[pl.ds(rows_y if dy == 1 else 1, 1)]

        def halo_copy(index, n):
            dz, dy = DIRS[n]
            return pltpu.make_async_remote_copy(
                src_ref=halo_source(index, dy),
                dst_ref=halo_slot(index, dz, dy),
                send_sem=halo_send.at[index, n],
                recv_sem=halo_recv.at[index, n],
                device_id=neighbour(dz, dy),
                device_id_type=MESH,
            )

        def halo_start(index):
            for n, (dz, dy) in enumerate(DIRS):
                @pl.when(exists(dz, dy))
                def _():
                    halo_copy(index, n).start()

        def halo_wait(index):
            for n, (dz, dy) in enumerate(DIRS):
                @pl.when(exists(-dz, -dy))
                def _():
                    halo_copy(index, n).wait_recv()

        def halo_drain(index):
            for n, (dz, dy) in enumerate(DIRS):
                @pl.when(exists(dz, dy))
                def _():
                    halo_copy(index, n).wait_send()

        view_peers = [{"view": lax.rem(v + k, views)} for k in range(1, views)]
        depth_peers = [{"depth": lax.rem(d + k, depths)} for k in range(1, depths)]
        me = h * views + v
        group_peers = []
        for k in range(1, group):
            to = lax.rem(me + k, group)
            group_peers.append((to, {"height": lax.div(to, views), "view": lax.rem(to, views)}))

        barrier = pltpu.get_barrier_semaphore()
        for dz, dy in DIRS:
            @pl.when(exists(dz, dy))
            def _():
                pl.semaphore_signal(barrier, inc=1, device_id=neighbour(dz, dy), device_id_type=MESH)
        for peer in view_peers + depth_peers + [p for _, p in group_peers]:
            pl.semaphore_signal(barrier, inc=1, device_id=peer, device_id_type=MESH)

        for dz, dy in DIRS:
            @pl.when(jnp.logical_not(exists(-dz, -dy)))
            def _():
                for index in range(6):
                    slot = halo_slot(index, dz, dy)
                    slot[...] = jnp.zeros(slot.shape, BF16)
        vol[OUTG, 1, pl.ds(1, rows_y)] = outg_ref[0]

        nrow = views * rows_y
        lane = lax.broadcasted_iota(jnp.int32, (1, tiles * channels), 1)
        row_id = lax.broadcasted_iota(jnp.int32, (nrow * channels, tiles * channels), 0)
        col_id = lax.broadcasted_iota(jnp.int32, (nrow * channels, tiles * channels), 1)
        same_channel = lax.rem(row_id, channels) == lax.rem(col_id, channels)
        target_id = jnp.where(same_channel, lax.div(row_id, channels), -1)
        lane_tile = lax.div(lane, channels)
        feats = feats_ref[...].reshape(tiles * channels, -1)
        partial = jnp.zeros((nrow * channels, width), F32)
        for k in range(slots):
            targets = jnp.zeros(lane.shape, jnp.int32)
            for t in range(tiles):
                targets = jnp.where(lane_tile == t, bricks_ref[t, k] * rows_y + rows_ref[t, k], targets)
            chosen = jnp.where(target_id == targets, 1.0, 0.0).astype(BF16)
            picked = jnp.dot(chosen, feats, preferred_element_type=F32).astype(BF16)
            partial += lax.dot_general(
                picked, foot_ref[k], (((1,), (1,)), ((), ())), preferred_element_type=F32
            )
        part[...] = partial.astype(BF16).reshape(views, rows_y, channels, width)

        count = len(view_peers) + len(depth_peers) + len(group_peers)
        for dz, dy in DIRS:
            count = count + exists(dz, dy).astype(jnp.int32)
        pl.semaphore_wait(barrier, count)

        def part_copy(k):
            to = lax.rem(v + k, views)
            return pltpu.make_async_remote_copy(
                src_ref=part.at[to], dst_ref=rsbuf.at[k],
                send_sem=view_send.at[0, k], recv_sem=view_recv.at[0, k],
                device_id={"view": to}, device_id_type=MESH,
            )

        for k in range(1, views):
            part_copy(k).start()
        halo_start(OUTG)

        def im2col(index):
            columns = []
            for y in range(rows_y):
                columns.append(jnp.concatenate(
                    [vol[index, a, pl.ds(y, 3)].reshape(srows, width) for a in range(3)], axis=0
                ))
            return jnp.concatenate(columns, axis=1)

        def to_rows(wide):
            return jnp.concatenate([wide[:, y * width:(y + 1) * width] for y in range(rows_y)], axis=0)

        def to_wide(tall):
            return jnp.concatenate([tall[y * channels:(y + 1) * channels] for y in range(rows_y)], axis=1)

        x_id = lax.broadcasted_iota(jnp.int32, (cells, width), 1)

        def from_left(values):
            return jnp.where(x_id == 0, 0.0, pltpu.roll(values, 1, 1))

        def from_right(values):
            return jnp.where(x_id == width - 1, 0.0, pltpu.roll(values, width - 1, 1))

        def conv(which, columns):
            taps = jnp.dot(w_ref[which], columns, preferred_element_type=F32)
            low, mid, high = (to_rows(taps[n * channels:(n + 1) * channels]) for n in range(3))
            return from_left(low) + mid + from_right(high)

        def grad_rows(grads):
            exact = grads.astype(F32)
            return [
                to_wide(from_right(exact).astype(BF16)),
                to_wide(grads),
                to_wide(from_left(exact).astype(BF16)),
            ]

        def weight_grad(columns, pieces):
            stacked = jnp.concatenate(pieces, axis=0)
            return lax.dot_general(columns, stacked, (((1,), (1,)), ((), ())), preferred_element_type=F32)

        def blank(rows):
            return jnp.zeros((rows, rows_y * width), BF16)

        def rows_sum(values):
            total = values[0:channels]
            for y in range(1, rows_y):
                total = total + values[y * channels:(y + 1) * channels]
            return total

        def tall_bias(n):
            return jnp.concatenate([bias_ref[n]] * rows_y, axis=0)

        def put(index, values):
            vol[index, 1, pl.ds(1, rows_y)] = values.reshape(rows_y, channels, width)

        outs = (early_out, late_out)

        def ar_a(n, k):
            to = lax.rem(d + k, depths)
            return pltpu.make_async_remote_copy(
                src_ref=own_sum.at[n, pl.ds(pl.multiple_of(to * piece, 8), piece)], dst_ref=ar_rs.at[n, k],
                send_sem=ar_send.at[n, 0, k], recv_sem=ar_recv.at[n, 0, k],
                device_id={"depth": to}, device_id_type=MESH,
            )

        def ar_b(n, k):
            to, peer = group_peers[k - 1]
            return pltpu.make_async_remote_copy(
                src_ref=ar_mid.at[n, me], dst_ref=ar_mid.at[n, me],
                send_sem=ar_send.at[n, 1, k], recv_sem=ar_recv.at[n, 1, k],
                device_id=peer, device_id_type=MESH,
            )

        def ar_b_in(n, k):
            source = lax.rem(me + group - k, group)
            return pltpu.make_async_remote_copy(
                src_ref=ar_mid.at[n, source], dst_ref=ar_mid.at[n, source],
                send_sem=ar_send.at[n, 1, k], recv_sem=ar_recv.at[n, 1, k],
                device_id=group_peers[k - 1][1], device_id_type=MESH,
            )

        def ar_c(n, k, owner):
            to = lax.rem(d + k, depths)
            place = outs[n].at[pl.ds(pl.multiple_of(owner * piece, 8), piece)]
            return pltpu.make_async_remote_copy(
                src_ref=place, dst_ref=place,
                send_sem=ar_send.at[n, 2, k], recv_sem=ar_recv.at[n, 2, k],
                device_id={"depth": to}, device_id_type=MESH,
            )

        def reduce_start(n, values, bias):
            own_sum[n, pl.ds(0, wrows)] = values
            own_sum[n, pl.ds(wrows, BIAS_ROWS)] = bias
            if depths * piece > total_rows:
                rest = depths * piece - total_rows
                own_sum[n, pl.ds(total_rows, rest)] = jnp.zeros((rest, 128), F32)
            for k in range(1, depths):
                ar_a(n, k).start()

        def reduce_middle(n):
            total = own_sum[n, pl.ds(pl.multiple_of(d * piece, 8), piece)]
            for k in range(1, depths):
                ar_a(n, k).wait_recv()
                total = total + ar_rs[n, k]
            ar_mid[n, me] = total
            for k in range(1, group):
                ar_b(n, k).start()

        def reduce_last(n):
            for k in range(1, group):
                ar_b_in(n, k).wait_recv()
            total = ar_mid[n, 0]
            for j in range(1, group):
                total = total + ar_mid[n, j]
            outs[n][pl.ds(pl.multiple_of(d * piece, 8), piece)] = total
            for k in range(1, depths):
                ar_c(n, k, d).start()

        def reduce_end(n):
            for k in range(1, depths):
                ar_c(n, k, lax.rem(d + depths - k, depths)).wait_recv()

        def reduce_drain(n):
            for k in range(1, depths):
                ar_a(n, k).wait_send()
                ar_c(n, k, d).wait_send()
            for k in range(1, group):
                ar_b(n, k).wait_send()

        lifted = part[v].astype(F32)
        for k in range(1, views):
            part_copy(k).wait_recv()
            lifted = lifted + rsbuf[k].astype(F32)
        put(LIFT, lifted.astype(BF16))
        halo_start(LIFT)

        halo_wait(OUTG)
        up_second = conv(3, im2col(OUTG))
        out_pieces = grad_rows(outg_ref[0].reshape(cells, width))

        halo_wait(LIFT)
        pre_first = conv(0, im2col(LIFT)) + tall_bias(0)
        act_first = jax.nn.silu(pre_first).astype(BF16)
        put(ACT1, act_first)
        halo_start(ACT1)
        slope_of_first = silu_grad(pre_first)

        halo_wait(ACT1)
        columns_second = im2col(ACT1)
        pre_second = conv(1, columns_second) + tall_bias(1)
        slope_second = up_second * silu_grad(pre_second)
        back_second = slope_second.astype(BF16)
        put(BACK2, back_second)
        halo_start(BACK2)
        act_second = (jax.nn.silu(pre_second) + act_first.astype(F32)).astype(BF16)
        put(ACT2, act_second)
        halo_start(ACT2)
        early = weight_grad(columns_second, grad_rows(back_second) + [blank(128 - srows)])

        halo_wait(BACK2)
        up_first = up_second + conv(4, im2col(BACK2))
        slope_first = up_first * slope_of_first
        back_first = slope_first.astype(BF16)
        put(BACK1, back_first)
        halo_start(BACK1)
        late = weight_grad(im2col(LIFT), grad_rows(back_first) + [blank(128 - srows)])
        reduce_start(1, late, rows_sum(slope_first))

        halo_wait(ACT2)
        columns_third = im2col(ACT2)
        field = conv(2, columns_third)
        field_ref[0] = field.astype(BF16).reshape(rows_y, channels, width)
        early = early + weight_grad(
            columns_third, [blank(srows)] + out_pieces + [blank(128 - 2 * srows)]
        )
        reduce_start(0, early, rows_sum(slope_second))

        halo_wait(BACK1)
        lift_grad = conv(5, im2col(BACK1)).astype(BF16)
        grid[v] = lift_grad.reshape(rows_y, channels, width)

        def grid_copy(k, place):
            return pltpu.make_async_remote_copy(
                src_ref=grid.at[place], dst_ref=grid.at[place],
                send_sem=view_send.at[1, k], recv_sem=view_recv.at[1, k],
                device_id={"view": lax.rem(v + k, views)}, device_id_type=MESH,
            )

        for k in range(1, views):
            grid_copy(k, v).start()
        reduce_middle(1)
        reduce_middle(0)
        for k in range(1, views):
            grid_copy(k, lax.rem(v + views - k, views)).wait_recv()
        reduce_last(1)
        reduce_last(0)
        camera = jnp.zeros((tiles * channels, width), F32)
        for k in range(slots):
            picked = jnp.concatenate(
                [grid[bricks_ref[t, k], rows_ref[t, k]] for t in range(tiles)], axis=0
            )
            camera += jnp.dot(picked, foot_ref[k], preferred_element_type=F32)
        camera_ref[...] = camera.reshape(tiles, channels, width)
        reduce_end(1)
        reduce_end(0)
        for index in range(6):
            halo_drain(index)
        for k in range(1, views):
            part_copy(k).wait_send()
            grid_copy(k, v).wait_send()
        for n in range(2):
            reduce_drain(n)

    vmem = pl.BlockSpec(memory_space=pltpu.VMEM)
    smem = pl.BlockSpec(memory_space=pltpu.SMEM)
    plane = (rows_y, channels, width)
    return pl.pallas_call(
        kernel,
        out_shape=(
            jax.ShapeDtypeStruct((1,) + plane, BF16),
            jax.ShapeDtypeStruct((tiles, channels, width), F32),
            jax.ShapeDtypeStruct((depths * piece, 128), F32),
            jax.ShapeDtypeStruct((depths * piece, 128), F32),
        ),
        in_specs=[smem, smem] + [vmem] * 5,
        out_specs=(vmem,) * 4,
        scratch_shapes=[
            pltpu.VMEM((6, 3, rows_y + 2, channels, width), BF16),
            pltpu.VMEM((views,) + plane, BF16),
            pltpu.VMEM((views,) + plane, BF16),
            pltpu.VMEM((views,) + plane, BF16),
            pltpu.VMEM((2, depths * piece, 128), F32),
            pltpu.VMEM((2, depths, piece, 128), F32),
            pltpu.VMEM((2, group, piece, 128), F32),
            pltpu.SemaphoreType.DMA((6, len(DIRS))),
            pltpu.SemaphoreType.DMA((6, len(DIRS))),
            pltpu.SemaphoreType.DMA((2, views)),
            pltpu.SemaphoreType.DMA((2, views)),
            pltpu.SemaphoreType.DMA((2, 3, max(depths, group))),
            pltpu.SemaphoreType.DMA((2, 3, max(depths, group))),
        ],
        compiler_params=pltpu.CompilerParams(collective_id=0, has_side_effects=True),
    )


def forward_matrix(weight):
    c = weight.shape[0]
    return jnp.transpose(weight, (4, 0, 2, 3, 1)).reshape(3 * c, 9 * c)


def backward_matrix(weight):
    c = weight.shape[0]
    return jnp.transpose(jnp.flip(weight, (2, 3, 4)), (4, 1, 2, 3, 0)).reshape(3 * c, 9 * c)


def body(
    camera_feats,
    footprint_slot_weights,
    tile_bricks,
    tile_rows,
    conv_first,
    conv_second,
    conv_third,
    bias_first,
    bias_second,
    out_grad,
):
    depths, heights, views = (lax.axis_size(a) for a in ("depth", "height", "view"))
    tiles, channels, _ = camera_feats.shape
    slots, width, _ = footprint_slot_weights.shape
    rows_y = out_grad.shape[1]
    weights = jnp.stack(
        [forward_matrix(w) for w in (conv_first, conv_second, conv_third)]
        + [backward_matrix(w) for w in (conv_third, conv_second, conv_first)]
    )
    biases = jnp.broadcast_to(
        jnp.stack([bias_first, bias_second])[:, :, None], (2, channels, width)
    )
    call = make_kernel(depths, heights, views, tiles, slots, rows_y, channels, width)
    field, camera, early, late = call(
        tile_bricks, tile_rows, camera_feats, footprint_slot_weights, weights, biases, out_grad
    )
    scale = 1.0 / math.sqrt(rows_y * width * depths * heights * views)
    wrows, srows = 9 * channels, 3 * channels
    parts = jnp.stack([late[:wrows, :srows], early[:wrows, :srows], early[:wrows, srows:2 * srows]])
    parts = parts.reshape(3, 3, 3, channels, 3, channels) * scale
    weight_grads = jnp.transpose(parts, (0, 5, 3, 1, 2, 4))
    sums = jnp.stack([late[wrows:wrows + channels], early[wrows:wrows + channels]])
    return field, camera, weight_grads, jnp.sum(sums, axis=2) * scale


def solution(mesh):
    in_specs = (
        P(("depth", "height", "view"), None, None),
        P(),
        P(("depth", "height", "view"), None),
        P(("depth", "height", "view"), None),
        P(),
        P(),
        P(),
        P(),
        P(),
        P(("depth", "view"), "height", None, None),
    )
    out_specs = (
        P(("depth", "view"), "height", None, None),
        P(("depth", "height", "view"), None, None),
        P(),
        P(),
    )
    return jax.shard_map(body, mesh=mesh, in_specs=in_specs, out_specs=out_specs, check_vma=False)
```

```python
import math

import jax
import jax.numpy as jnp
from jax import lax
from jax.experimental import pallas as pl
from jax.experimental.pallas import tpu as pltpu
from jax.sharding import PartitionSpec as P

MESH = pl.DeviceIdType.MESH
F32 = jnp.float32
BF16 = jnp.bfloat16
DIRS = [(dz, dy) for dz in (-1, 0, 1) for dy in (0, -1, 1) if (dz, dy) != (0, 0)]
LIFT, ACT1, ACT2, OUTG, BACK2, BACK1 = range(6)
PARAMS = {"vmem_limit_bytes": 16 * 1024 * 1024}


def round_up(value, step):
    return -(-value // step) * step


def silu_grad(values):
    sigma = jax.nn.sigmoid(values)
    return sigma * (1.0 + values * (1.0 - sigma))


def make_kernel(depths, heights, views, tiles, slots, rows_y, channels, width):
    group = heights * views
    wrows = 9 * channels
    srows = 3 * channels
    cells = rows_y * channels
    half = 2 * srows
    sizes = (2 * half, half)
    pieces = tuple(round_up(-(-size // depths), 8) for size in sizes)
    piece_max = max(pieces)

    def kernel(
        bricks_ref, rows_ref, feats_ref, foot_ref, w1_ref, w2_ref, w3_ref, bias1_ref, bias2_ref, outg_ref,
        field_ref, camera_ref, early_out, late_out,
        w_ref, vol, part, rsbuf, grid, own_sum, ar_rs, ar_mid,
        halo_send, halo_recv, view_send, view_recv, ar_send, ar_recv,
    ):
        d = lax.axis_index("depth")
        h = lax.axis_index("height")
        v = lax.axis_index("view")
        z = d * views + v
        planes = depths * views

        def exists(dz, dy):
            tests = []
            if dz == -1:
                tests.append(z > 0)
            if dz == 1:
                tests.append(z < planes - 1)
            if dy == -1:
                tests.append(h > 0)
            if dy == 1:
                tests.append(h < heights - 1)
            result = tests[0]
            for test in tests[1:]:
                result = jnp.logical_and(result, test)
            return result

        def neighbour(dz, dy):
            to = z + dz
            return {"depth": lax.div(to, views), "view": lax.rem(to, views), "height": h + dy}

        def halo_slot(index, dz, dy):
            if dy == 0:
                return vol.at[index, 1 - dz, pl.ds(1, rows_y)]
            return vol.at[index, 1 - dz, pl.ds(0 if dy == 1 else rows_y + 1, 1)]

        def halo_source(index, dy):
            base = vol.at[index, 1]
            if dy == 0:
                return base.at[pl.ds(1, rows_y)]
            return base.at[pl.ds(rows_y if dy == 1 else 1, 1)]

        def halo_copy(index, n):
            dz, dy = DIRS[n]
            return pltpu.make_async_remote_copy(
                src_ref=halo_source(index, dy),
                dst_ref=halo_slot(index, dz, dy),
                send_sem=halo_send.at[index, n],
                recv_sem=halo_recv.at[index, n],
                device_id=neighbour(dz, dy),
                device_id_type=MESH,
            )

        def halo_start(index):
            for n, (dz, dy) in enumerate(DIRS):
                @pl.when(exists(dz, dy))
                def _():
                    halo_copy(index, n).start()

        def halo_wait(index):
            for n, (dz, dy) in enumerate(DIRS):
                @pl.when(exists(-dz, -dy))
                def _():
                    halo_copy(index, n).wait_recv()

        def halo_drain(index):
            for n, (dz, dy) in enumerate(DIRS):
                @pl.when(exists(dz, dy))
                def _():
                    halo_copy(index, n).wait_send()

        view_peers = [{"view": lax.rem(v + k, views)} for k in range(1, views)]
        depth_peers = [{"depth": lax.rem(d + k, depths)} for k in range(1, depths)]
        me = h * views + v
        group_peers = []
        for k in range(1, group):
            to = lax.rem(me + k, group)
            group_peers.append((to, {"height": lax.div(to, views), "view": lax.rem(to, views)}))

        barrier = pltpu.get_barrier_semaphore()
        for dz, dy in DIRS:
            @pl.when(exists(dz, dy))
            def _():
                pl.semaphore_signal(barrier, inc=1, device_id=neighbour(dz, dy), device_id_type=MESH)
        for peer in view_peers + depth_peers + [p for _, p in group_peers]:
            pl.semaphore_signal(barrier, inc=1, device_id=peer, device_id_type=MESH)

        for dz, dy in DIRS:
            @pl.when(jnp.logical_not(exists(-dz, -dy)))
            def _():
                for index in range(6):
                    slot = halo_slot(index, dz, dy)
                    slot[...] = jnp.zeros(slot.shape, BF16)
        vol[OUTG, 1, pl.ds(1, rows_y)] = outg_ref[0]

        nrow = views * rows_y
        lane = lax.broadcasted_iota(jnp.int32, (1, tiles * channels), 1)
        row_id = lax.broadcasted_iota(jnp.int32, (nrow * channels, tiles * channels), 0)
        col_id = lax.broadcasted_iota(jnp.int32, (nrow * channels, tiles * channels), 1)
        same_channel = lax.rem(row_id, channels) == lax.rem(col_id, channels)
        target_id = jnp.where(same_channel, lax.div(row_id, channels), -1)
        lane_tile = lax.div(lane, channels)
        feats = feats_ref[...].reshape(tiles * channels, -1)
        partial = jnp.zeros((nrow * channels, width), F32)
        for k in range(slots):
            targets = jnp.zeros(lane.shape, jnp.int32)
            for t in range(tiles):
                targets = jnp.where(lane_tile == t, bricks_ref[t, k] * rows_y + rows_ref[t, k], targets)
            chosen = jnp.where(target_id == targets, 1.0, 0.0).astype(BF16)
            picked = jnp.dot(chosen, feats, preferred_element_type=F32).astype(BF16)
            partial += lax.dot_general(
                picked, foot_ref[k], (((1,), (1,)), ((), ())), preferred_element_type=F32
            )
        part[...] = partial.astype(BF16).reshape(views, rows_y, channels, width)

        count = len(view_peers) + len(depth_peers) + len(group_peers)
        for dz, dy in DIRS:
            count = count + exists(dz, dy).astype(jnp.int32)
        pl.semaphore_wait(barrier, count)

        def part_copy(k):
            to = lax.rem(v + k, views)
            return pltpu.make_async_remote_copy(
                src_ref=part.at[to], dst_ref=rsbuf.at[k],
                send_sem=view_send.at[0, k], recv_sem=view_recv.at[0, k],
                device_id={"view": to}, device_id_type=MESH,
            )

        for k in range(1, views):
            part_copy(k).start()
        halo_start(OUTG)

        for n, ref in enumerate((w1_ref, w2_ref, w3_ref)):
            tiles_f = [ref[t].astype(F32) for t in range(27)]
            ahead = [jnp.concatenate([tiles_f[3 * ab + c] for c in range(3)], axis=0) for ab in range(9)]
            w_ref[n] = jnp.concatenate(ahead, axis=1).astype(BF16)
            back = [jnp.concatenate([tiles_f[26 - 3 * ab - c] for ab in range(9)], axis=0) for c in range(3)]
            w_ref[5 - n] = jnp.concatenate([tile.T for tile in back], axis=0).astype(BF16)

        def im2col(index):
            columns = []
            for y in range(rows_y):
                columns.append(jnp.concatenate(
                    [vol[index, a, pl.ds(y, 3)].reshape(srows, width) for a in range(3)], axis=0
                ))
            return jnp.concatenate(columns, axis=1)

        def to_rows(wide):
            return jnp.concatenate([wide[:, y * width:(y + 1) * width] for y in range(rows_y)], axis=0)

        def to_wide(tall):
            return jnp.concatenate([tall[y * channels:(y + 1) * channels] for y in range(rows_y)], axis=1)

        x_id = lax.broadcasted_iota(jnp.int32, (cells, width), 1)

        def from_left(values):
            return jnp.where(x_id == 0, 0.0, pltpu.roll(values, 1, 1))

        def from_right(values):
            return jnp.where(x_id == width - 1, 0.0, pltpu.roll(values, width - 1, 1))

        def conv(which, columns):
            taps = jnp.dot(w_ref[which], columns, preferred_element_type=F32)
            low, mid, high = (to_rows(taps[n * channels:(n + 1) * channels]) for n in range(3))
            return from_left(low) + mid + from_right(high)

        def grad_rows(grads):
            exact = grads.astype(F32)
            return [
                to_wide(from_right(exact).astype(BF16)),
                to_wide(grads),
                to_wide(from_left(exact).astype(BF16)),
            ]

        def weight_grad(columns, pieces):
            stacked = jnp.concatenate(pieces, axis=0)
            return lax.dot_general(stacked, columns, (((1,), (1,)), ((), ())), preferred_element_type=F32)

        def rows_sum(values):
            total = values[0:channels]
            for y in range(1, rows_y):
                total = total + values[y * channels:(y + 1) * channels]
            return jnp.sum(total, axis=1, keepdims=True)

        def tall_bias(ref):
            shape = (cells, channels)
            diagonal = lax.rem(lax.broadcasted_iota(jnp.int32, shape, 0), channels)
            diagonal = diagonal == lax.broadcasted_iota(jnp.int32, shape, 1)
            spread = jnp.broadcast_to(ref[...], shape)
            return jnp.sum(jnp.where(diagonal, spread, 0.0), axis=1, keepdims=True)

        def put(index, values):
            vol[index, 1, pl.ds(1, rows_y)] = values.reshape(rows_y, channels, width)

        outs = (early_out, late_out)

        def ar_a(n, k):
            to = lax.rem(d + k, depths)
            return pltpu.make_async_remote_copy(
                src_ref=own_sum.at[n, pl.ds(pl.multiple_of(to * pieces[n], 8), pieces[n])], dst_ref=ar_rs.at[n, k, pl.ds(0, pieces[n])],
                send_sem=ar_send.at[n, 0, k], recv_sem=ar_recv.at[n, 0, k],
                device_id={"depth": to}, device_id_type=MESH,
            )

        def ar_b(n, k):
            to, peer = group_peers[k - 1]
            return pltpu.make_async_remote_copy(
                src_ref=ar_mid.at[n, me, pl.ds(0, pieces[n])], dst_ref=ar_mid.at[n, me, pl.ds(0, pieces[n])],
                send_sem=ar_send.at[n, 1, k], recv_sem=ar_recv.at[n, 1, k],
                device_id=peer, device_id_type=MESH,
            )

        def ar_b_in(n, k):
            source = lax.rem(me + group - k, group)
            return pltpu.make_async_remote_copy(
                src_ref=ar_mid.at[n, source, pl.ds(0, pieces[n])], dst_ref=ar_mid.at[n, source, pl.ds(0, pieces[n])],
                send_sem=ar_send.at[n, 1, k], recv_sem=ar_recv.at[n, 1, k],
                device_id=group_peers[k - 1][1], device_id_type=MESH,
            )

        def ar_c(n, k, owner):
            to = lax.rem(d + k, depths)
            place = outs[n].at[pl.ds(pl.multiple_of(owner * pieces[n], 8), pieces[n])]
            return pltpu.make_async_remote_copy(
                src_ref=place, dst_ref=place,
                send_sem=ar_send.at[n, 2, k], recv_sem=ar_recv.at[n, 2, k],
                device_id={"depth": to}, device_id_type=MESH,
            )

        def keep_grad(n, base, values, bias=None):
            main = 128
            own_sum[n, pl.ds(base, srows)] = values[:, :main]
            own_sum[n, pl.ds(base + srows, srows)] = jnp.zeros((srows, 128), F32)
            own_sum[n, pl.ds(base + srows, srows), pl.ds(0, wrows - main)] = values[:, main:]
            if bias is not None:
                place = pl.ds(base + srows, channels)
                lanes = lax.broadcasted_iota(jnp.int32, (channels, 128), 1)
                own_sum[n, place] = jnp.where(lanes == wrows - main, bias, own_sum[n, place])

        def reduce_start(n):
            rest = depths * pieces[n] - sizes[n]
            if rest:
                own_sum[n, pl.ds(sizes[n], rest)] = jnp.zeros((rest, 128), F32)
            for k in range(1, depths):
                ar_a(n, k).start()

        def reduce_middle(n):
            total = own_sum[n, pl.ds(pl.multiple_of(d * pieces[n], 8), pieces[n])]
            for k in range(1, depths):
                ar_a(n, k).wait_recv()
                total = total + ar_rs[n, k, pl.ds(0, pieces[n])]
            ar_mid[n, me, pl.ds(0, pieces[n])] = total
            for k in range(1, group):
                ar_b(n, k).start()

        def reduce_last(n):
            for k in range(1, group):
                ar_b_in(n, k).wait_recv()
            total = ar_mid[n, 0, pl.ds(0, pieces[n])]
            for j in range(1, group):
                total = total + ar_mid[n, j, pl.ds(0, pieces[n])]
            outs[n][pl.ds(pl.multiple_of(d * pieces[n], 8), pieces[n])] = total
            for k in range(1, depths):
                ar_c(n, k, d).start()

        def reduce_end(n):
            for k in range(1, depths):
                ar_c(n, k, lax.rem(d + depths - k, depths)).wait_recv()

        def reduce_drain(n):
            for k in range(1, depths):
                ar_a(n, k).wait_send()
                ar_c(n, k, d).wait_send()
            for k in range(1, group):
                ar_b(n, k).wait_send()

        lifted = part[v].astype(F32)
        for k in range(1, views):
            part_copy(k).wait_recv()
            lifted = lifted + rsbuf[k].astype(F32)
        put(LIFT, lifted.astype(BF16))
        halo_start(LIFT)

        halo_wait(OUTG)
        up_second = conv(3, im2col(OUTG))
        out_pieces = grad_rows(outg_ref[0].reshape(cells, width))

        halo_wait(LIFT)
        pre_first = conv(0, im2col(LIFT)) + tall_bias(bias1_ref)
        act_first = jax.nn.silu(pre_first).astype(BF16)
        put(ACT1, act_first)
        halo_start(ACT1)
        slope_of_first = silu_grad(pre_first)

        halo_wait(ACT1)
        columns_second = im2col(ACT1)
        pre_second = conv(1, columns_second) + tall_bias(bias2_ref)
        slope_second = up_second * silu_grad(pre_second)
        back_second = slope_second.astype(BF16)
        put(BACK2, back_second)
        halo_start(BACK2)
        act_second = (jax.nn.silu(pre_second) + act_first.astype(F32)).astype(BF16)
        put(ACT2, act_second)
        halo_start(ACT2)
        early = weight_grad(columns_second, grad_rows(back_second))
        keep_grad(0, 0, early, rows_sum(slope_second))

        halo_wait(BACK2)
        up_first = up_second + conv(4, im2col(BACK2))
        slope_first = up_first * slope_of_first
        back_first = slope_first.astype(BF16)
        put(BACK1, back_first)
        halo_start(BACK1)
        late = weight_grad(im2col(LIFT), grad_rows(back_first))
        keep_grad(1, 0, late, rows_sum(slope_first))
        reduce_start(1)

        halo_wait(ACT2)
        columns_third = im2col(ACT2)
        field = conv(2, columns_third)
        field_ref[0] = field.astype(BF16).reshape(rows_y, channels, width)
        keep_grad(0, half, weight_grad(columns_third, out_pieces))
        reduce_start(0)

        halo_wait(BACK1)
        lift_grad = conv(5, im2col(BACK1)).astype(BF16)
        grid[v] = lift_grad.reshape(rows_y, channels, width)

        def grid_copy(k, place):
            return pltpu.make_async_remote_copy(
                src_ref=grid.at[place], dst_ref=grid.at[place],
                send_sem=view_send.at[1, k], recv_sem=view_recv.at[1, k],
                device_id={"view": lax.rem(v + k, views)}, device_id_type=MESH,
            )

        for k in range(1, views):
            grid_copy(k, v).start()
        reduce_middle(1)
        reduce_middle(0)
        for k in range(1, views):
            grid_copy(k, lax.rem(v + views - k, views)).wait_recv()
        reduce_last(1)
        reduce_last(0)
        camera = jnp.zeros((tiles * channels, width), F32)
        for k in range(slots):
            picked = jnp.concatenate(
                [grid[bricks_ref[t, k], rows_ref[t, k]] for t in range(tiles)], axis=0
            )
            camera += jnp.dot(picked, foot_ref[k], preferred_element_type=F32)
        camera_ref[...] = camera.reshape(tiles, channels, width)
        reduce_end(1)
        reduce_end(0)
        for index in range(6):
            halo_drain(index)
        for k in range(1, views):
            part_copy(k).wait_send()
            grid_copy(k, v).wait_send()
        for n in range(2):
            reduce_drain(n)

    vmem = pl.BlockSpec(memory_space=pltpu.VMEM)
    smem = pl.BlockSpec(memory_space=pltpu.SMEM)
    plane = (rows_y, channels, width)
    return pl.pallas_call(
        kernel,
        out_shape=(
            jax.ShapeDtypeStruct((1,) + plane, BF16),
            jax.ShapeDtypeStruct((tiles, channels, width), F32),
            jax.ShapeDtypeStruct((depths * pieces[0], 128), F32),
            jax.ShapeDtypeStruct((depths * pieces[1], 128), F32),
        ),
        in_specs=[smem, smem] + [vmem] * 8,
        out_specs=(vmem,) * 4,
        scratch_shapes=[
            pltpu.VMEM((6, srows, wrows), BF16),
            pltpu.VMEM((6, 3, rows_y + 2, channels, width), BF16),
            pltpu.VMEM((views,) + plane, BF16),
            pltpu.VMEM((views,) + plane, BF16),
            pltpu.VMEM((views,) + plane, BF16),
            pltpu.VMEM((2, depths * piece_max, 128), F32),
            pltpu.VMEM((2, depths, piece_max, 128), F32),
            pltpu.VMEM((2, group, piece_max, 128), F32),
            pltpu.SemaphoreType.DMA((6, len(DIRS))),
            pltpu.SemaphoreType.DMA((6, len(DIRS))),
            pltpu.SemaphoreType.DMA((2, views)),
            pltpu.SemaphoreType.DMA((2, views)),
            pltpu.SemaphoreType.DMA((2, 3, max(depths, group))),
            pltpu.SemaphoreType.DMA((2, 3, max(depths, group))),
        ],
        compiler_params=pltpu.CompilerParams(collective_id=0, has_side_effects=True, **PARAMS),
    )


def finish(field, camera, early, late, scale, channels):
    wrows, srows = 9 * channels, 3 * channels

    def kernel(field_in, camera_in, early_ref, late_ref, field_ref, camera_ref, grads_ref, bias_ref):
        field_ref[...] = field_in[...]
        camera_ref[...] = camera_in[...]
        per_row = 128 // channels
        for n, (ref, base) in enumerate(((late_ref, 0), (early_ref, 0), (early_ref, 2 * srows))):
            for ab in range(9):
                rows = base + srows * (ab // per_row)
                lanes = channels * (ab % per_row)
                tile = ref[pl.ds(rows, srows), pl.ds(lanes, channels)] * scale
                for c in range(3):
                    grads_ref[n, 3 * ab + c] = tile[c * channels:(c + 1) * channels]
            if n < 2:
                column = ref[pl.ds(base + srows, channels), pl.ds(wrows - 128, 1)] * scale
                shape = (channels, channels)
                diagonal = lax.broadcasted_iota(jnp.int32, shape, 0) == lax.broadcasted_iota(jnp.int32, shape, 1)
                spread = jnp.where(diagonal, jnp.broadcast_to(column, shape), 0.0)
                bias_ref[pl.ds(n, 1)] = jnp.sum(spread, axis=0, keepdims=True)

    vmem = pl.BlockSpec(memory_space=pltpu.VMEM)
    return pl.pallas_call(
        kernel,
        out_shape=(
            jax.ShapeDtypeStruct(field.shape, field.dtype),
            jax.ShapeDtypeStruct(camera.shape, camera.dtype),
            jax.ShapeDtypeStruct((3, 27, channels, channels), F32),
            jax.ShapeDtypeStruct((2, channels), F32),
        ),
        in_specs=[vmem] * 4,
        out_specs=(vmem,) * 4,
        compiler_params=pltpu.CompilerParams(**PARAMS),
    )(field, camera, early, late)


def tap_tiles(weight):
    c = weight.shape[0]
    return jnp.transpose(weight, (2, 3, 4, 0, 1)).reshape(27, c, c)


def body(
    camera_feats,
    footprint_slot_weights,
    tile_bricks,
    tile_rows,
    conv_first,
    conv_second,
    conv_third,
    bias_first,
    bias_second,
    out_grad,
):
    depths, heights, views = (lax.axis_size(a) for a in ("depth", "height", "view"))
    tiles, channels, _ = camera_feats.shape
    slots, width, _ = footprint_slot_weights.shape
    rows_y = out_grad.shape[1]
    call = make_kernel(depths, heights, views, tiles, slots, rows_y, channels, width)
    field, camera, early, late = call(
        tile_bricks, tile_rows, camera_feats, footprint_slot_weights,
        tap_tiles(conv_first), tap_tiles(conv_second), tap_tiles(conv_third),
        bias_first[None], bias_second[None], out_grad,
    )
    scale = 1.0 / math.sqrt(rows_y * width * depths * heights * views)
    field, camera, grads, biases = finish(field, camera, early, late, scale, channels)
    grads = grads.reshape(3, 3, 3, 3, channels, channels)
    return field, camera, jnp.transpose(grads, (0, 4, 5, 1, 2, 3)), biases


def solution(mesh):
    in_specs = (
        P(("depth", "height", "view"), None, None),
        P(),
        P(("depth", "height", "view"), None),
        P(("depth", "height", "view"), None),
        P(),
        P(),
        P(),
        P(),
        P(),
        P(("depth", "view"), "height", None, None),
    )
    out_specs = (
        P(("depth", "view"), "height", None, None),
        P(("depth", "height", "view"), None, None),
        P(),
        P(),
    )
    return jax.shard_map(body, mesh=mesh, in_specs=in_specs, out_specs=out_specs, check_vma=False)
```

```python
import math

import jax
import jax.numpy as jnp
from jax import lax
from jax.experimental import pallas as pl
from jax.experimental.pallas import tpu as pltpu
from jax.sharding import PartitionSpec as P

MESH = pl.DeviceIdType.MESH
F32 = jnp.float32
BF16 = jnp.bfloat16
DIRS = [(dz, dy) for dz in (-1, 0, 1) for dy in (0, -1, 1) if (dz, dy) != (0, 0)]
LIFT, ACT1, ACT2, OUTG, BACK2, BACK1 = range(6)
PARAMS = {"vmem_limit_bytes": 65150 * 1024}


def round_up(value, step):
    return -(-value // step) * step


def silu_grad(values):
    sigma = jax.nn.sigmoid(values)
    return sigma * (1.0 + values * (1.0 - sigma))


def make_kernel(depths, heights, views, tiles, slots, rows_y, channels, width):
    group = heights * views
    wrows = 9 * channels
    srows = 3 * channels
    cells = rows_y * channels
    half = 2 * srows
    sizes = (2 * half, half)
    pieces = tuple(round_up(-(-size // depths), 8) for size in sizes)
    piece_max = max(pieces)

    def kernel(
        bricks_hbm, rows_hbm, feats_hbm, foot_hbm, w1_hbm, w2_hbm, w3_hbm, bias1_hbm, bias2_hbm, outg_hbm,
        field_ref, camera_ref, early_out, late_out,
        bricks_ref, rows_ref, feats_ref, foot_ref, w1_ref, w2_ref, w3_ref, bias1_ref, bias2_ref, in_sem,
        w_ref, vol, part, rsbuf, grid, own_sum, ar_rs, ar_mid,
        halo_send, halo_recv, view_send, view_recv, ar_send, ar_recv,
    ):
        sources = (
            bricks_hbm, rows_hbm, feats_hbm, foot_hbm, outg_hbm.at[0],
            w1_hbm, w2_hbm, w3_hbm, bias1_hbm, bias2_hbm,
        )
        places = (
            bricks_ref, rows_ref, feats_ref, foot_ref, vol.at[OUTG, 1, pl.ds(1, rows_y)],
            w1_ref, w2_ref, w3_ref, bias1_ref, bias2_ref,
        )
        loads = [
            pltpu.make_async_copy(source, place, in_sem.at[n])
            for n, (source, place) in enumerate(zip(sources, places))
        ]
        for load in loads:
            load.start()
        d = lax.axis_index("depth")
        h = lax.axis_index("height")
        v = lax.axis_index("view")
        z = d * views + v
        planes = depths * views

        def exists(dz, dy):
            tests = []
            if dz == -1:
                tests.append(z > 0)
            if dz == 1:
                tests.append(z < planes - 1)
            if dy == -1:
                tests.append(h > 0)
            if dy == 1:
                tests.append(h < heights - 1)
            result = tests[0]
            for test in tests[1:]:
                result = jnp.logical_and(result, test)
            return result

        def neighbour(dz, dy):
            to = z + dz
            return {"depth": lax.div(to, views), "view": lax.rem(to, views), "height": h + dy}

        def halo_slot(index, dz, dy):
            if dy == 0:
                return vol.at[index, 1 - dz, pl.ds(1, rows_y)]
            return vol.at[index, 1 - dz, pl.ds(0 if dy == 1 else rows_y + 1, 1)]

        def halo_source(index, dy):
            base = vol.at[index, 1]
            if dy == 0:
                return base.at[pl.ds(1, rows_y)]
            return base.at[pl.ds(rows_y if dy == 1 else 1, 1)]

        def halo_copy(index, n):
            dz, dy = DIRS[n]
            return pltpu.make_async_remote_copy(
                src_ref=halo_source(index, dy),
                dst_ref=halo_slot(index, dz, dy),
                send_sem=halo_send.at[index, n],
                recv_sem=halo_recv.at[index, n],
                device_id=neighbour(dz, dy),
                device_id_type=MESH,
            )

        def halo_start(index):
            for n, (dz, dy) in enumerate(DIRS):
                @pl.when(exists(dz, dy))
                def _():
                    halo_copy(index, n).start()

        def halo_wait(index):
            for n, (dz, dy) in enumerate(DIRS):
                @pl.when(exists(-dz, -dy))
                def _():
                    halo_copy(index, n).wait_recv()

        def halo_drain(index):
            for n, (dz, dy) in enumerate(DIRS):
                @pl.when(exists(dz, dy))
                def _():
                    halo_copy(index, n).wait_send()

        view_peers = [{"view": lax.rem(v + k, views)} for k in range(1, views)]
        depth_peers = [{"depth": lax.rem(d + k, depths)} for k in range(1, depths)]
        me = h * views + v
        group_peers = []
        for k in range(1, group):
            to = lax.rem(me + k, group)
            group_peers.append((to, {"height": lax.div(to, views), "view": lax.rem(to, views)}))

        barrier = pltpu.get_barrier_semaphore()
        for dz, dy in DIRS:
            @pl.when(exists(dz, dy))
            def _():
                pl.semaphore_signal(barrier, inc=1, device_id=neighbour(dz, dy), device_id_type=MESH)
        for peer in view_peers + depth_peers + [p for _, p in group_peers]:
            pl.semaphore_signal(barrier, inc=1, device_id=peer, device_id_type=MESH)

        for dz, dy in DIRS:
            @pl.when(jnp.logical_not(exists(-dz, -dy)))
            def _():
                for index in range(6):
                    slot = halo_slot(index, dz, dy)
                    slot[...] = jnp.zeros(slot.shape, BF16)
        for load in loads[:4]:
            load.wait()

        nrow = views * rows_y
        lane = lax.broadcasted_iota(jnp.int32, (1, tiles * channels), 1)
        row_id = lax.broadcasted_iota(jnp.int32, (nrow * channels, tiles * channels), 0)
        col_id = lax.broadcasted_iota(jnp.int32, (nrow * channels, tiles * channels), 1)
        same_channel = lax.rem(row_id, channels) == lax.rem(col_id, channels)
        target_id = jnp.where(same_channel, lax.div(row_id, channels), -1)
        lane_tile = lax.div(lane, channels)
        feats = feats_ref[...].reshape(tiles * channels, -1)
        partial = jnp.zeros((nrow * channels, width), F32)
        for k in range(slots):
            targets = jnp.zeros(lane.shape, jnp.int32)
            for t in range(tiles):
                targets = jnp.where(lane_tile == t, bricks_ref[t, k] * rows_y + rows_ref[t, k], targets)
            chosen = jnp.where(target_id == targets, 1.0, 0.0).astype(BF16)
            picked = jnp.dot(chosen, feats, preferred_element_type=F32).astype(BF16)
            partial += lax.dot_general(
                picked, foot_ref[k], (((1,), (1,)), ((), ())), preferred_element_type=F32
            )
        part[...] = partial.astype(BF16).reshape(views, rows_y, channels, width)

        count = len(view_peers) + len(depth_peers) + len(group_peers)
        for dz, dy in DIRS:
            count = count + exists(dz, dy).astype(jnp.int32)
        pl.semaphore_wait(barrier, count)

        def part_copy(k):
            to = lax.rem(v + k, views)
            return pltpu.make_async_remote_copy(
                src_ref=part.at[to], dst_ref=rsbuf.at[k],
                send_sem=view_send.at[0, k], recv_sem=view_recv.at[0, k],
                device_id={"view": to}, device_id_type=MESH,
            )

        for k in range(1, views):
            part_copy(k).start()
        loads[4].wait()
        halo_start(OUTG)
        for load in loads[5:]:
            load.wait()

        for n, ref in enumerate((w1_ref, w2_ref, w3_ref)):
            tiles_f = [ref[t].astype(F32) for t in range(27)]
            ahead = [jnp.concatenate([tiles_f[3 * ab + c] for c in range(3)], axis=0) for ab in range(9)]
            w_ref[n] = jnp.concatenate(ahead, axis=1).astype(BF16)
            back = [jnp.concatenate([tiles_f[26 - 3 * ab - c] for ab in range(9)], axis=0) for c in range(3)]
            w_ref[5 - n] = jnp.concatenate([tile.T for tile in back], axis=0).astype(BF16)

        def im2col(index):
            columns = []
            for y in range(rows_y):
                columns.append(jnp.concatenate(
                    [vol[index, a, pl.ds(y, 3)].reshape(srows, width) for a in range(3)], axis=0
                ))
            return jnp.concatenate(columns, axis=1)

        def to_rows(wide):
            return jnp.concatenate([wide[:, y * width:(y + 1) * width] for y in range(rows_y)], axis=0)

        def to_wide(tall):
            return jnp.concatenate([tall[y * channels:(y + 1) * channels] for y in range(rows_y)], axis=1)

        x_id = lax.broadcasted_iota(jnp.int32, (cells, width), 1)

        def from_left(values):
            return jnp.where(x_id == 0, 0.0, pltpu.roll(values, 1, 1))

        def from_right(values):
            return jnp.where(x_id == width - 1, 0.0, pltpu.roll(values, width - 1, 1))

        def conv(which, columns):
            taps = jnp.dot(w_ref[which], columns, preferred_element_type=F32)
            low, mid, high = (to_rows(taps[n * channels:(n + 1) * channels]) for n in range(3))
            return from_left(low) + mid + from_right(high)

        def grad_rows(grads):
            exact = grads.astype(F32)
            return [
                to_wide(from_right(exact).astype(BF16)),
                to_wide(grads),
                to_wide(from_left(exact).astype(BF16)),
            ]

        def weight_grad(columns, pieces):
            stacked = jnp.concatenate(pieces, axis=0)
            return lax.dot_general(stacked, columns, (((1,), (1,)), ((), ())), preferred_element_type=F32)

        def rows_sum(values):
            total = values[0:channels]
            for y in range(1, rows_y):
                total = total + values[y * channels:(y + 1) * channels]
            return jnp.sum(total, axis=1, keepdims=True)

        def tall_bias(ref):
            shape = (cells, channels)
            diagonal = lax.rem(lax.broadcasted_iota(jnp.int32, shape, 0), channels)
            diagonal = diagonal == lax.broadcasted_iota(jnp.int32, shape, 1)
            spread = jnp.broadcast_to(ref[...], shape)
            return jnp.sum(jnp.where(diagonal, spread, 0.0), axis=1, keepdims=True)

        def put(index, values):
            vol[index, 1, pl.ds(1, rows_y)] = values.reshape(rows_y, channels, width)

        outs = (early_out, late_out)

        def ar_a(n, k):
            to = lax.rem(d + k, depths)
            return pltpu.make_async_remote_copy(
                src_ref=own_sum.at[n, pl.ds(pl.multiple_of(to * pieces[n], 8), pieces[n])], dst_ref=ar_rs.at[n, k, pl.ds(0, pieces[n])],
                send_sem=ar_send.at[n, 0, k], recv_sem=ar_recv.at[n, 0, k],
                device_id={"depth": to}, device_id_type=MESH,
            )

        def ar_b(n, k):
            to, peer = group_peers[k - 1]
            return pltpu.make_async_remote_copy(
                src_ref=ar_mid.at[n, me, pl.ds(0, pieces[n])], dst_ref=ar_mid.at[n, me, pl.ds(0, pieces[n])],
                send_sem=ar_send.at[n, 1, k], recv_sem=ar_recv.at[n, 1, k],
                device_id=peer, device_id_type=MESH,
            )

        def ar_b_in(n, k):
            source = lax.rem(me + group - k, group)
            return pltpu.make_async_remote_copy(
                src_ref=ar_mid.at[n, source, pl.ds(0, pieces[n])], dst_ref=ar_mid.at[n, source, pl.ds(0, pieces[n])],
                send_sem=ar_send.at[n, 1, k], recv_sem=ar_recv.at[n, 1, k],
                device_id=group_peers[k - 1][1], device_id_type=MESH,
            )

        def ar_c(n, k, owner):
            to = lax.rem(d + k, depths)
            place = outs[n].at[pl.ds(pl.multiple_of(owner * pieces[n], 8), pieces[n])]
            return pltpu.make_async_remote_copy(
                src_ref=place, dst_ref=place,
                send_sem=ar_send.at[n, 2, k], recv_sem=ar_recv.at[n, 2, k],
                device_id={"depth": to}, device_id_type=MESH,
            )

        def keep_grad(n, base, values, bias=None):
            main = 128
            own_sum[n, pl.ds(base, srows)] = values[:, :main]
            own_sum[n, pl.ds(base + srows, srows)] = jnp.zeros((srows, 128), F32)
            own_sum[n, pl.ds(base + srows, srows), pl.ds(0, wrows - main)] = values[:, main:]
            if bias is not None:
                place = pl.ds(base + srows, channels)
                lanes = lax.broadcasted_iota(jnp.int32, (channels, 128), 1)
                own_sum[n, place] = jnp.where(lanes == wrows - main, bias, own_sum[n, place])

        def reduce_start(n):
            rest = depths * pieces[n] - sizes[n]
            if rest:
                own_sum[n, pl.ds(sizes[n], rest)] = jnp.zeros((rest, 128), F32)
            for k in range(1, depths):
                ar_a(n, k).start()

        def reduce_middle(n):
            total = own_sum[n, pl.ds(pl.multiple_of(d * pieces[n], 8), pieces[n])]
            for k in range(1, depths):
                ar_a(n, k).wait_recv()
                total = total + ar_rs[n, k, pl.ds(0, pieces[n])]
            ar_mid[n, me, pl.ds(0, pieces[n])] = total
            for k in range(1, group):
                ar_b(n, k).start()

        def reduce_last(n):
            for k in range(1, group):
                ar_b_in(n, k).wait_recv()
            total = ar_mid[n, 0, pl.ds(0, pieces[n])]
            for j in range(1, group):
                total = total + ar_mid[n, j, pl.ds(0, pieces[n])]
            outs[n][pl.ds(pl.multiple_of(d * pieces[n], 8), pieces[n])] = total
            for k in range(1, depths):
                ar_c(n, k, d).start()

        def reduce_end(n):
            for k in range(1, depths):
                ar_c(n, k, lax.rem(d + depths - k, depths)).wait_recv()

        def reduce_drain(n):
            for k in range(1, depths):
                ar_a(n, k).wait_send()
                ar_c(n, k, d).wait_send()
            for k in range(1, group):
                ar_b(n, k).wait_send()

        lifted = part[v].astype(F32)
        for k in range(1, views):
            part_copy(k).wait_recv()
            lifted = lifted + rsbuf[k].astype(F32)
        put(LIFT, lifted.astype(BF16))
        halo_start(LIFT)

        halo_wait(OUTG)
        up_second = conv(3, im2col(OUTG))
        out_pieces = grad_rows(vol[OUTG, 1, pl.ds(1, rows_y)].reshape(cells, width))

        halo_wait(LIFT)
        pre_first = conv(0, im2col(LIFT)) + tall_bias(bias1_ref)
        act_first = jax.nn.silu(pre_first).astype(BF16)
        put(ACT1, act_first)
        halo_start(ACT1)
        slope_of_first = silu_grad(pre_first)

        halo_wait(ACT1)
        columns_second = im2col(ACT1)
        pre_second = conv(1, columns_second) + tall_bias(bias2_ref)
        slope_second = up_second * silu_grad(pre_second)
        back_second = slope_second.astype(BF16)
        put(BACK2, back_second)
        halo_start(BACK2)
        act_second = (jax.nn.silu(pre_second) + act_first.astype(F32)).astype(BF16)
        put(ACT2, act_second)
        halo_start(ACT2)
        early = weight_grad(columns_second, grad_rows(back_second))
        keep_grad(0, 0, early, rows_sum(slope_second))

        halo_wait(BACK2)
        up_first = up_second + conv(4, im2col(BACK2))
        slope_first = up_first * slope_of_first
        back_first = slope_first.astype(BF16)
        put(BACK1, back_first)
        halo_start(BACK1)
        late = weight_grad(im2col(LIFT), grad_rows(back_first))
        keep_grad(1, 0, late, rows_sum(slope_first))
        reduce_start(1)

        halo_wait(ACT2)
        columns_third = im2col(ACT2)
        field = conv(2, columns_third)
        field_ref[0] = field.astype(BF16).reshape(rows_y, channels, width)
        keep_grad(0, half, weight_grad(columns_third, out_pieces))
        reduce_start(0)

        halo_wait(BACK1)
        lift_grad = conv(5, im2col(BACK1)).astype(BF16)
        grid[v] = lift_grad.reshape(rows_y, channels, width)

        def grid_copy(k, place):
            return pltpu.make_async_remote_copy(
                src_ref=grid.at[place], dst_ref=grid.at[place],
                send_sem=view_send.at[1, k], recv_sem=view_recv.at[1, k],
                device_id={"view": lax.rem(v + k, views)}, device_id_type=MESH,
            )

        for k in range(1, views):
            grid_copy(k, v).start()
        reduce_middle(1)
        reduce_middle(0)
        for k in range(1, views):
            grid_copy(k, lax.rem(v + views - k, views)).wait_recv()
        reduce_last(1)
        reduce_last(0)
        camera = jnp.zeros((tiles * channels, width), F32)
        for k in range(slots):
            picked = jnp.concatenate(
                [grid[bricks_ref[t, k], rows_ref[t, k]] for t in range(tiles)], axis=0
            )
            camera += jnp.dot(picked, foot_ref[k], preferred_element_type=F32)
        camera_ref[...] = camera.reshape(tiles, channels, width)
        reduce_end(1)
        reduce_end(0)
        for index in range(6):
            halo_drain(index)
        for k in range(1, views):
            part_copy(k).wait_send()
            grid_copy(k, v).wait_send()
        for n in range(2):
            reduce_drain(n)

    vmem = pl.BlockSpec(memory_space=pltpu.VMEM)
    hbm = pl.BlockSpec(memory_space=pltpu.HBM)
    plane = (rows_y, channels, width)
    return pl.pallas_call(
        kernel,
        out_shape=(
            jax.ShapeDtypeStruct((1,) + plane, BF16),
            jax.ShapeDtypeStruct((tiles, channels, width), F32),
            jax.ShapeDtypeStruct((depths * pieces[0], 128), F32),
            jax.ShapeDtypeStruct((depths * pieces[1], 128), F32),
        ),
        in_specs=[hbm] * 10,
        out_specs=(vmem,) * 4,
        scratch_shapes=[
            pltpu.SMEM((tiles, slots), jnp.int32),
            pltpu.SMEM((tiles, slots), jnp.int32),
            pltpu.VMEM((tiles, channels, width), BF16),
            pltpu.VMEM((slots, width, width), BF16),
            pltpu.VMEM((27, channels, channels), BF16),
            pltpu.VMEM((27, channels, channels), BF16),
            pltpu.VMEM((27, channels, channels), BF16),
            pltpu.VMEM((1, channels), F32),
            pltpu.VMEM((1, channels), F32),
            pltpu.SemaphoreType.DMA((10,)),
            pltpu.VMEM((6, srows, wrows), BF16),
            pltpu.VMEM((6, 3, rows_y + 2, channels, width), BF16),
            pltpu.VMEM((views,) + plane, BF16),
            pltpu.VMEM((views,) + plane, BF16),
            pltpu.VMEM((views,) + plane, BF16),
            pltpu.VMEM((2, depths * piece_max, 128), F32),
            pltpu.VMEM((2, depths, piece_max, 128), F32),
            pltpu.VMEM((2, group, piece_max, 128), F32),
            pltpu.SemaphoreType.DMA((6, len(DIRS))),
            pltpu.SemaphoreType.DMA((6, len(DIRS))),
            pltpu.SemaphoreType.DMA((2, views)),
            pltpu.SemaphoreType.DMA((2, views)),
            pltpu.SemaphoreType.DMA((2, 3, max(depths, group))),
            pltpu.SemaphoreType.DMA((2, 3, max(depths, group))),
        ],
        compiler_params=pltpu.CompilerParams(collective_id=0, has_side_effects=True, **PARAMS),
    )


def finish(field, camera, early, late, scale, channels):
    wrows, srows = 9 * channels, 3 * channels

    def kernel(field_in, camera_in, early_ref, late_ref, field_ref, camera_ref, grads_ref, bias_ref):
        field_ref[...] = field_in[...]
        camera_ref[...] = camera_in[...]
        per_row = 128 // channels
        for n, (ref, base) in enumerate(((late_ref, 0), (early_ref, 0), (early_ref, 2 * srows))):
            for ab in range(9):
                rows = base + srows * (ab // per_row)
                lanes = channels * (ab % per_row)
                tile = ref[pl.ds(rows, srows), pl.ds(lanes, channels)] * scale
                for c in range(3):
                    grads_ref[n, 3 * ab + c] = tile[c * channels:(c + 1) * channels]
            if n < 2:
                column = ref[pl.ds(base + srows, channels), pl.ds(wrows - 128, 1)] * scale
                shape = (channels, channels)
                diagonal = lax.broadcasted_iota(jnp.int32, shape, 0) == lax.broadcasted_iota(jnp.int32, shape, 1)
                spread = jnp.where(diagonal, jnp.broadcast_to(column, shape), 0.0)
                bias_ref[pl.ds(n, 1)] = jnp.sum(spread, axis=0, keepdims=True)

    vmem = pl.BlockSpec(memory_space=pltpu.VMEM)
    return pl.pallas_call(
        kernel,
        out_shape=(
            jax.ShapeDtypeStruct(field.shape, field.dtype),
            jax.ShapeDtypeStruct(camera.shape, camera.dtype),
            jax.ShapeDtypeStruct((3, 27, channels, channels), F32),
            jax.ShapeDtypeStruct((2, channels), F32),
        ),
        in_specs=[vmem] * 4,
        out_specs=(vmem,) * 4,
        compiler_params=pltpu.CompilerParams(**PARAMS),
    )(field, camera, early, late)


def tap_tiles(weight):
    c = weight.shape[0]
    return jnp.transpose(weight, (2, 3, 4, 0, 1)).reshape(27, c, c)


def body(
    camera_feats,
    footprint_slot_weights,
    tile_bricks,
    tile_rows,
    conv_first,
    conv_second,
    conv_third,
    bias_first,
    bias_second,
    out_grad,
):
    depths, heights, views = (lax.axis_size(a) for a in ("depth", "height", "view"))
    tiles, channels, _ = camera_feats.shape
    slots, width, _ = footprint_slot_weights.shape
    rows_y = out_grad.shape[1]
    call = make_kernel(depths, heights, views, tiles, slots, rows_y, channels, width)
    field, camera, early, late = call(
        tile_bricks, tile_rows, camera_feats, footprint_slot_weights,
        tap_tiles(conv_first), tap_tiles(conv_second), tap_tiles(conv_third),
        bias_first[None], bias_second[None], out_grad,
    )
    scale = 1.0 / math.sqrt(rows_y * width * depths * heights * views)
    field, camera, grads, biases = finish(field, camera, early, late, scale, channels)
    grads = grads.reshape(3, 3, 3, 3, channels, channels)
    return field, camera, jnp.transpose(grads, (0, 4, 5, 1, 2, 3)), biases


def solution(mesh):
    in_specs = (
        P(("depth", "height", "view"), None, None),
        P(),
        P(("depth", "height", "view"), None),
        P(("depth", "height", "view"), None),
        P(),
        P(),
        P(),
        P(),
        P(),
        P(("depth", "view"), "height", None, None),
    )
    out_specs = (
        P(("depth", "view"), "height", None, None),
        P(("depth", "height", "view"), None, None),
        P(),
        P(),
    )
    return jax.shard_map(body, mesh=mesh, in_specs=in_specs, out_specs=out_specs, check_vma=False)
```

```python
import math

import jax
import jax.numpy as jnp
from jax import lax
from jax.experimental import pallas as pl
from jax.experimental.pallas import tpu as pltpu
from jax.sharding import PartitionSpec as P

MESH = pl.DeviceIdType.MESH
F32 = jnp.float32
BF16 = jnp.bfloat16
DIRS = [(dz, dy) for dz in (-1, 0, 1) for dy in (0, -1, 1) if (dz, dy) != (0, 0)]
LIFT, ACT1, ACT2, OUTG, BACK2, BACK1 = range(6)
PARAMS = {"vmem_limit_bytes": 65150 * 1024}


def round_up(value, step):
    return -(-value // step) * step


def silu_grad(values):
    sigma = jax.nn.sigmoid(values)
    return sigma * (1.0 + values * (1.0 - sigma))


def make_kernel(depths, heights, views, tiles, slots, rows_y, channels, width):
    group = heights * views
    wrows = 9 * channels
    srows = 3 * channels
    cells = rows_y * channels
    half = 2 * srows
    sizes = (2 * half, half)
    pieces = tuple(round_up(-(-size // depths), 8) for size in sizes)
    piece_max = max(pieces)

    def kernel(
        bricks_hbm, rows_hbm, feats_hbm, foot_hbm, w1_hbm, w2_hbm, w3_hbm, bias1_hbm, bias2_hbm, outg_hbm,
        field_ref, camera_ref, early_out, late_out,
        bricks_ref, rows_ref, feats_ref, foot_ref, w1_ref, w2_ref, w3_ref, bias1_ref, bias2_ref, in_sem,
        outg_ref, field_own, field_in, swap_send, swap_recv, w_ref, vol, part, rsbuf, grid, own_sum, ar_rs, ar_mid,
        halo_send, halo_recv, view_send, view_recv, ar_send, ar_recv,
    ):
        sources = (
            bricks_hbm, rows_hbm, feats_hbm, foot_hbm, outg_hbm.at[0],
            w1_hbm, w2_hbm, w3_hbm, bias1_hbm, bias2_hbm,
        )
        places = (
            bricks_ref, rows_ref, feats_ref, foot_ref, outg_ref,
            w1_ref, w2_ref, w3_ref, bias1_ref, bias2_ref,
        )
        loads = [
            pltpu.make_async_copy(source, place, in_sem.at[n])
            for n, (source, place) in enumerate(zip(sources, places))
        ]
        for load in loads:
            load.start()
        d = lax.axis_index("depth")
        h = lax.axis_index("height")
        v = lax.axis_index("view")

        def turn(depth, view):
            return jnp.where(lax.rem(depth, 2) == 1, views - 1 - view, view)

        brick = turn(d, v)
        moved = brick != v
        z = d * views + brick
        planes = depths * views

        def exists(dz, dy):
            tests = []
            if dz == -1:
                tests.append(z > 0)
            if dz == 1:
                tests.append(z < planes - 1)
            if dy == -1:
                tests.append(h > 0)
            if dy == 1:
                tests.append(h < heights - 1)
            result = tests[0]
            for test in tests[1:]:
                result = jnp.logical_and(result, test)
            return result

        def neighbour(dz, dy):
            to = z + dz
            row = lax.div(to, views)
            return {"depth": row, "view": turn(row, lax.rem(to, views)), "height": h + dy}

        def halo_slot(index, dz, dy):
            if dy == 0:
                return vol.at[index, 1 - dz, pl.ds(1, rows_y)]
            return vol.at[index, 1 - dz, pl.ds(0 if dy == 1 else rows_y + 1, 1)]

        def halo_source(index, dy):
            base = vol.at[index, 1]
            if dy == 0:
                return base.at[pl.ds(1, rows_y)]
            return base.at[pl.ds(rows_y if dy == 1 else 1, 1)]

        def halo_copy(index, n):
            dz, dy = DIRS[n]
            return pltpu.make_async_remote_copy(
                src_ref=halo_source(index, dy),
                dst_ref=halo_slot(index, dz, dy),
                send_sem=halo_send.at[index, n],
                recv_sem=halo_recv.at[index, n],
                device_id=neighbour(dz, dy),
                device_id_type=MESH,
            )

        def halo_start(index):
            for n, (dz, dy) in enumerate(DIRS):
                @pl.when(exists(dz, dy))
                def _():
                    halo_copy(index, n).start()

        def halo_wait(index):
            for n, (dz, dy) in enumerate(DIRS):
                @pl.when(exists(-dz, -dy))
                def _():
                    halo_copy(index, n).wait_recv()

        def halo_drain(index):
            for n, (dz, dy) in enumerate(DIRS):
                @pl.when(exists(dz, dy))
                def _():
                    halo_copy(index, n).wait_send()

        view_peers = [{"view": lax.rem(v + k, views)} for k in range(1, views)]
        depth_peers = [{"depth": lax.rem(d + k, depths)} for k in range(1, depths)]
        me = h * views + v
        group_peers = []
        for k in range(1, group):
            to = lax.rem(me + k, group)
            group_peers.append((to, {"height": lax.div(to, views), "view": lax.rem(to, views)}))

        barrier = pltpu.get_barrier_semaphore()
        for dz, dy in DIRS:
            @pl.when(exists(dz, dy))
            def _():
                pl.semaphore_signal(barrier, inc=1, device_id=neighbour(dz, dy), device_id_type=MESH)
        for peer in view_peers + depth_peers + [p for _, p in group_peers]:
            pl.semaphore_signal(barrier, inc=1, device_id=peer, device_id_type=MESH)

        for dz, dy in DIRS:
            @pl.when(jnp.logical_not(exists(-dz, -dy)))
            def _():
                for index in range(6):
                    slot = halo_slot(index, dz, dy)
                    slot[...] = jnp.zeros(slot.shape, BF16)
        for load in loads[:4]:
            load.wait()

        nrow = views * rows_y
        lane = lax.broadcasted_iota(jnp.int32, (1, tiles * channels), 1)
        row_id = lax.broadcasted_iota(jnp.int32, (nrow * channels, tiles * channels), 0)
        col_id = lax.broadcasted_iota(jnp.int32, (nrow * channels, tiles * channels), 1)
        same_channel = lax.rem(row_id, channels) == lax.rem(col_id, channels)
        target_id = jnp.where(same_channel, lax.div(row_id, channels), -1)
        lane_tile = lax.div(lane, channels)
        feats = feats_ref[...].reshape(tiles * channels, -1)
        partial = jnp.zeros((nrow * channels, width), F32)
        for k in range(slots):
            targets = jnp.zeros(lane.shape, jnp.int32)
            for t in range(tiles):
                targets = jnp.where(lane_tile == t, bricks_ref[t, k] * rows_y + rows_ref[t, k], targets)
            chosen = jnp.where(target_id == targets, 1.0, 0.0).astype(BF16)
            picked = jnp.dot(chosen, feats, preferred_element_type=F32).astype(BF16)
            partial += lax.dot_general(
                picked, foot_ref[k], (((1,), (1,)), ((), ())), preferred_element_type=F32
            )
        part[...] = partial.astype(BF16).reshape(views, rows_y, channels, width)

        count = len(view_peers) + len(depth_peers) + len(group_peers)
        for dz, dy in DIRS:
            count = count + exists(dz, dy).astype(jnp.int32)
        pl.semaphore_wait(barrier, count)

        def part_copy(k):
            to = lax.rem(v + k, views)
            return pltpu.make_async_remote_copy(
                src_ref=part.at[turn(d, to)], dst_ref=rsbuf.at[k],
                send_sem=view_send.at[0, k], recv_sem=view_recv.at[0, k],
                device_id={"view": to}, device_id_type=MESH,
            )

        for k in range(1, views):
            part_copy(k).start()
        for load in loads[4:]:
            load.wait()

        def swap_copy(n):
            return pltpu.make_async_remote_copy(
                src_ref=(outg_ref, field_own)[n],
                dst_ref=(vol.at[OUTG, 1, pl.ds(1, rows_y)], field_in)[n],
                send_sem=swap_send.at[n], recv_sem=swap_recv.at[n],
                device_id={"view": brick}, device_id_type=MESH,
            )

        @pl.when(moved)
        def _():
            swap_copy(0).start()

        @pl.when(jnp.logical_not(moved))
        def _():
            vol[OUTG, 1, pl.ds(1, rows_y)] = outg_ref[...]

        for n, ref in enumerate((w1_ref, w2_ref, w3_ref)):
            tiles_f = [ref[t].astype(F32) for t in range(27)]
            ahead = [jnp.concatenate([tiles_f[3 * ab + c] for c in range(3)], axis=0) for ab in range(9)]
            w_ref[n] = jnp.concatenate(ahead, axis=1).astype(BF16)
            back = [jnp.concatenate([tiles_f[26 - 3 * ab - c] for ab in range(9)], axis=0) for c in range(3)]
            w_ref[5 - n] = jnp.concatenate([tile.T for tile in back], axis=0).astype(BF16)

        def im2col(index):
            columns = []
            for y in range(rows_y):
                columns.append(jnp.concatenate(
                    [vol[index, a, pl.ds(y, 3)].reshape(srows, width) for a in range(3)], axis=0
                ))
            return jnp.concatenate(columns, axis=1)

        def to_rows(wide):
            return jnp.concatenate([wide[:, y * width:(y + 1) * width] for y in range(rows_y)], axis=0)

        def to_wide(tall):
            return jnp.concatenate([tall[y * channels:(y + 1) * channels] for y in range(rows_y)], axis=1)

        x_id = lax.broadcasted_iota(jnp.int32, (cells, width), 1)

        def from_left(values):
            return jnp.where(x_id == 0, 0.0, pltpu.roll(values, 1, 1))

        def from_right(values):
            return jnp.where(x_id == width - 1, 0.0, pltpu.roll(values, width - 1, 1))

        def conv(which, columns):
            taps = jnp.dot(w_ref[which], columns, preferred_element_type=F32)
            low, mid, high = (to_rows(taps[n * channels:(n + 1) * channels]) for n in range(3))
            return from_left(low) + mid + from_right(high)

        def grad_rows(grads):
            exact = grads.astype(F32)
            return [
                to_wide(from_right(exact).astype(BF16)),
                to_wide(grads),
                to_wide(from_left(exact).astype(BF16)),
            ]

        def weight_grad(columns, pieces):
            stacked = jnp.concatenate(pieces, axis=0)
            return lax.dot_general(stacked, columns, (((1,), (1,)), ((), ())), preferred_element_type=F32)

        def rows_sum(values):
            total = values[0:channels]
            for y in range(1, rows_y):
                total = total + values[y * channels:(y + 1) * channels]
            return jnp.sum(total, axis=1, keepdims=True)

        def tall_bias(ref):
            shape = (cells, channels)
            diagonal = lax.rem(lax.broadcasted_iota(jnp.int32, shape, 0), channels)
            diagonal = diagonal == lax.broadcasted_iota(jnp.int32, shape, 1)
            spread = jnp.broadcast_to(ref[...], shape)
            return jnp.sum(jnp.where(diagonal, spread, 0.0), axis=1, keepdims=True)

        def put(index, values):
            vol[index, 1, pl.ds(1, rows_y)] = values.reshape(rows_y, channels, width)

        outs = (early_out, late_out)

        def ar_a(n, k):
            to = lax.rem(d + k, depths)
            return pltpu.make_async_remote_copy(
                src_ref=own_sum.at[n, pl.ds(pl.multiple_of(to * pieces[n], 8), pieces[n])], dst_ref=ar_rs.at[n, k, pl.ds(0, pieces[n])],
                send_sem=ar_send.at[n, 0, k], recv_sem=ar_recv.at[n, 0, k],
                device_id={"depth": to}, device_id_type=MESH,
            )

        def ar_b(n, k):
            to, peer = group_peers[k - 1]
            return pltpu.make_async_remote_copy(
                src_ref=ar_mid.at[n, me, pl.ds(0, pieces[n])], dst_ref=ar_mid.at[n, me, pl.ds(0, pieces[n])],
                send_sem=ar_send.at[n, 1, k], recv_sem=ar_recv.at[n, 1, k],
                device_id=peer, device_id_type=MESH,
            )

        def ar_b_in(n, k):
            source = lax.rem(me + group - k, group)
            return pltpu.make_async_remote_copy(
                src_ref=ar_mid.at[n, source, pl.ds(0, pieces[n])], dst_ref=ar_mid.at[n, source, pl.ds(0, pieces[n])],
                send_sem=ar_send.at[n, 1, k], recv_sem=ar_recv.at[n, 1, k],
                device_id=group_peers[k - 1][1], device_id_type=MESH,
            )

        def ar_c(n, k, owner):
            to = lax.rem(d + k, depths)
            place = outs[n].at[pl.ds(pl.multiple_of(owner * pieces[n], 8), pieces[n])]
            return pltpu.make_async_remote_copy(
                src_ref=place, dst_ref=place,
                send_sem=ar_send.at[n, 2, k], recv_sem=ar_recv.at[n, 2, k],
                device_id={"depth": to}, device_id_type=MESH,
            )

        def keep_grad(n, base, values, bias=None):
            main = 128
            own_sum[n, pl.ds(base, srows)] = values[:, :main]
            own_sum[n, pl.ds(base + srows, srows)] = jnp.zeros((srows, 128), F32)
            own_sum[n, pl.ds(base + srows, srows), pl.ds(0, wrows - main)] = values[:, main:]
            if bias is not None:
                place = pl.ds(base + srows, channels)
                lanes = lax.broadcasted_iota(jnp.int32, (channels, 128), 1)
                own_sum[n, place] = jnp.where(lanes == wrows - main, bias, own_sum[n, place])

        def reduce_start(n):
            rest = depths * pieces[n] - sizes[n]
            if rest:
                own_sum[n, pl.ds(sizes[n], rest)] = jnp.zeros((rest, 128), F32)
            for k in range(1, depths):
                ar_a(n, k).start()

        def reduce_middle(n):
            total = own_sum[n, pl.ds(pl.multiple_of(d * pieces[n], 8), pieces[n])]
            for k in range(1, depths):
                ar_a(n, k).wait_recv()
                total = total + ar_rs[n, k, pl.ds(0, pieces[n])]
            ar_mid[n, me, pl.ds(0, pieces[n])] = total
            for k in range(1, group):
                ar_b(n, k).start()

        def reduce_last(n):
            for k in range(1, group):
                ar_b_in(n, k).wait_recv()
            total = ar_mid[n, 0, pl.ds(0, pieces[n])]
            for j in range(1, group):
                total = total + ar_mid[n, j, pl.ds(0, pieces[n])]
            outs[n][pl.ds(pl.multiple_of(d * pieces[n], 8), pieces[n])] = total
            for k in range(1, depths):
                ar_c(n, k, d).start()

        def reduce_end(n):
            for k in range(1, depths):
                ar_c(n, k, lax.rem(d + depths - k, depths)).wait_recv()

        def reduce_drain(n):
            for k in range(1, depths):
                ar_a(n, k).wait_send()
                ar_c(n, k, d).wait_send()
            for k in range(1, group):
                ar_b(n, k).wait_send()

        lifted = part[brick].astype(F32)
        for k in range(1, views):
            part_copy(k).wait_recv()
            lifted = lifted + rsbuf[k].astype(F32)
        put(LIFT, lifted.astype(BF16))
        halo_start(LIFT)

        @pl.when(moved)
        def _():
            swap_copy(0).wait_recv()

        halo_start(OUTG)
        halo_wait(LIFT)
        columns_first = im2col(LIFT)
        pre_first = conv(0, columns_first) + tall_bias(bias1_ref)
        act_first = jax.nn.silu(pre_first).astype(BF16)
        put(ACT1, act_first)
        halo_start(ACT1)
        slope_of_first = silu_grad(pre_first)

        halo_wait(OUTG)
        up_second = conv(3, im2col(OUTG))
        out_pieces = grad_rows(vol[OUTG, 1, pl.ds(1, rows_y)].reshape(cells, width))

        halo_wait(ACT1)
        columns_second = im2col(ACT1)
        pre_second = conv(1, columns_second) + tall_bias(bias2_ref)
        slope_second = up_second * silu_grad(pre_second)
        back_second = slope_second.astype(BF16)
        put(BACK2, back_second)
        halo_start(BACK2)
        act_second = (jax.nn.silu(pre_second) + act_first.astype(F32)).astype(BF16)
        put(ACT2, act_second)
        halo_start(ACT2)
        early = weight_grad(columns_second, grad_rows(back_second))
        keep_grad(0, 0, early, rows_sum(slope_second))

        halo_wait(BACK2)
        up_first = up_second + conv(4, im2col(BACK2))
        slope_first = up_first * slope_of_first
        back_first = slope_first.astype(BF16)
        put(BACK1, back_first)
        halo_start(BACK1)
        late = weight_grad(im2col(LIFT), grad_rows(back_first))
        keep_grad(1, 0, late, rows_sum(slope_first))
        reduce_start(1)

        halo_wait(ACT2)
        columns_third = im2col(ACT2)
        field = conv(2, columns_third)
        field_own[...] = field.astype(BF16).reshape(rows_y, channels, width)

        @pl.when(moved)
        def _():
            swap_copy(1).start()

        keep_grad(0, half, weight_grad(columns_third, out_pieces))
        reduce_start(0)

        halo_wait(BACK1)
        lift_grad = conv(5, im2col(BACK1)).astype(BF16)
        grid[brick] = lift_grad.reshape(rows_y, channels, width)

        def grid_copy(k, place):
            return pltpu.make_async_remote_copy(
                src_ref=grid.at[place], dst_ref=grid.at[place],
                send_sem=view_send.at[1, k], recv_sem=view_recv.at[1, k],
                device_id={"view": lax.rem(v + k, views)}, device_id_type=MESH,
            )

        for k in range(1, views):
            grid_copy(k, brick).start()
        reduce_middle(1)
        reduce_middle(0)
        for k in range(1, views):
            grid_copy(k, turn(d, lax.rem(v + views - k, views))).wait_recv()
        reduce_last(1)
        reduce_last(0)
        camera = jnp.zeros((tiles * channels, width), F32)
        for k in range(slots):
            picked = jnp.concatenate(
                [grid[bricks_ref[t, k], rows_ref[t, k]] for t in range(tiles)], axis=0
            )
            camera += jnp.dot(picked, foot_ref[k], preferred_element_type=F32)
        camera_ref[...] = camera.reshape(tiles, channels, width)
        @pl.when(moved)
        def _():
            swap_copy(1).wait_recv()
            field_ref[0] = field_in[...]
            for n in range(2):
                swap_copy(n).wait_send()

        @pl.when(jnp.logical_not(moved))
        def _():
            field_ref[0] = field_own[...]

        reduce_end(1)
        reduce_end(0)
        for index in range(6):
            halo_drain(index)
        for k in range(1, views):
            part_copy(k).wait_send()
            grid_copy(k, brick).wait_send()
        for n in range(2):
            reduce_drain(n)

    vmem = pl.BlockSpec(memory_space=pltpu.VMEM)
    hbm = pl.BlockSpec(memory_space=pltpu.HBM)
    plane = (rows_y, channels, width)
    return pl.pallas_call(
        kernel,
        out_shape=(
            jax.ShapeDtypeStruct((1,) + plane, BF16),
            jax.ShapeDtypeStruct((tiles, channels, width), F32),
            jax.ShapeDtypeStruct((depths * pieces[0], 128), F32),
            jax.ShapeDtypeStruct((depths * pieces[1], 128), F32),
        ),
        in_specs=[hbm] * 10,
        out_specs=(vmem,) * 4,
        scratch_shapes=[
            pltpu.SMEM((tiles, slots), jnp.int32),
            pltpu.SMEM((tiles, slots), jnp.int32),
            pltpu.VMEM((tiles, channels, width), BF16),
            pltpu.VMEM((slots, width, width), BF16),
            pltpu.VMEM((27, channels, channels), BF16),
            pltpu.VMEM((27, channels, channels), BF16),
            pltpu.VMEM((27, channels, channels), BF16),
            pltpu.VMEM((1, channels), F32),
            pltpu.VMEM((1, channels), F32),
            pltpu.SemaphoreType.DMA((10,)),
            pltpu.VMEM(plane, BF16),
            pltpu.VMEM(plane, BF16),
            pltpu.VMEM(plane, BF16),
            pltpu.SemaphoreType.DMA((2,)),
            pltpu.SemaphoreType.DMA((2,)),
            pltpu.VMEM((6, srows, wrows), BF16),
            pltpu.VMEM((6, 3, rows_y + 2, channels, width), BF16),
            pltpu.VMEM((views,) + plane, BF16),
            pltpu.VMEM((views,) + plane, BF16),
            pltpu.VMEM((views,) + plane, BF16),
            pltpu.VMEM((2, depths * piece_max, 128), F32),
            pltpu.VMEM((2, depths, piece_max, 128), F32),
            pltpu.VMEM((2, group, piece_max, 128), F32),
            pltpu.SemaphoreType.DMA((6, len(DIRS))),
            pltpu.SemaphoreType.DMA((6, len(DIRS))),
            pltpu.SemaphoreType.DMA((2, views)),
            pltpu.SemaphoreType.DMA((2, views)),
            pltpu.SemaphoreType.DMA((2, 3, max(depths, group))),
            pltpu.SemaphoreType.DMA((2, 3, max(depths, group))),
        ],
        compiler_params=pltpu.CompilerParams(collective_id=0, has_side_effects=True, **PARAMS),
    )


def finish(field, camera, early, late, scale, channels):
    wrows, srows = 9 * channels, 3 * channels

    def kernel(field_in, camera_in, early_ref, late_ref, field_ref, camera_ref, grads_ref, bias_ref):
        field_ref[...] = field_in[...]
        camera_ref[...] = camera_in[...]
        per_row = 128 // channels
        for n, (ref, base) in enumerate(((late_ref, 0), (early_ref, 0), (early_ref, 2 * srows))):
            for ab in range(9):
                rows = base + srows * (ab // per_row)
                lanes = channels * (ab % per_row)
                tile = ref[pl.ds(rows, srows), pl.ds(lanes, channels)] * scale
                for c in range(3):
                    grads_ref[n, 3 * ab + c] = tile[c * channels:(c + 1) * channels]
            if n < 2:
                column = ref[pl.ds(base + srows, channels), pl.ds(wrows - 128, 1)] * scale
                shape = (channels, channels)
                diagonal = lax.broadcasted_iota(jnp.int32, shape, 0) == lax.broadcasted_iota(jnp.int32, shape, 1)
                spread = jnp.where(diagonal, jnp.broadcast_to(column, shape), 0.0)
                bias_ref[pl.ds(n, 1)] = jnp.sum(spread, axis=0, keepdims=True)

    vmem = pl.BlockSpec(memory_space=pltpu.VMEM)
    return pl.pallas_call(
        kernel,
        out_shape=(
            jax.ShapeDtypeStruct(field.shape, field.dtype),
            jax.ShapeDtypeStruct(camera.shape, camera.dtype),
            jax.ShapeDtypeStruct((3, 27, channels, channels), F32),
            jax.ShapeDtypeStruct((2, channels), F32),
        ),
        in_specs=[vmem] * 4,
        out_specs=(vmem,) * 4,
        compiler_params=pltpu.CompilerParams(**PARAMS),
    )(field, camera, early, late)


def tap_tiles(weight):
    c = weight.shape[0]
    return jnp.transpose(weight, (2, 3, 4, 0, 1)).reshape(27, c, c)


def body(
    camera_feats,
    footprint_slot_weights,
    tile_bricks,
    tile_rows,
    conv_first,
    conv_second,
    conv_third,
    bias_first,
    bias_second,
    out_grad,
):
    depths, heights, views = (lax.axis_size(a) for a in ("depth", "height", "view"))
    tiles, channels, _ = camera_feats.shape
    slots, width, _ = footprint_slot_weights.shape
    rows_y = out_grad.shape[1]
    call = make_kernel(depths, heights, views, tiles, slots, rows_y, channels, width)
    field, camera, early, late = call(
        tile_bricks, tile_rows, camera_feats, footprint_slot_weights,
        tap_tiles(conv_first), tap_tiles(conv_second), tap_tiles(conv_third),
        bias_first[None], bias_second[None], out_grad,
    )
    scale = 1.0 / math.sqrt(rows_y * width * depths * heights * views)
    field, camera, grads, biases = finish(field, camera, early, late, scale, channels)
    grads = grads.reshape(3, 3, 3, 3, channels, channels)
    return field, camera, jnp.transpose(grads, (0, 4, 5, 1, 2, 3)), biases


def solution(mesh):
    in_specs = (
        P(("depth", "height", "view"), None, None),
        P(),
        P(("depth", "height", "view"), None),
        P(("depth", "height", "view"), None),
        P(),
        P(),
        P(),
        P(),
        P(),
        P(("depth", "view"), "height", None, None),
    )
    out_specs = (
        P(("depth", "view"), "height", None, None),
        P(("depth", "height", "view"), None, None),
        P(),
        P(),
    )
    return jax.shard_map(body, mesh=mesh, in_specs=in_specs, out_specs=out_specs, check_vma=False)
```
